32 devices in a mesh: grp: 4 (over z), ep: 8 (over y, x, core).
Axes of the slice: x: 2, y: 2, z: 4, core: 2. Of those that a mesh axis runs over, the one named last changes fastest.
Arguments:
- hidden: bfloat16 [4, 8, 32, 1024], P('grp', 'ep'), may hold values from -6 to 6
- down_weight: bfloat16 [8, 1024, 4096], P('ep'), may hold values from -0.1875 to 0.1875
- slot_gate: float32 [4, 8, 32], P('grp', 'ep'), may hold values from 0.02 to 0.6
- slot_owner: int32 [4, 8, 32], P('grp', 'ep'), may hold values from 0 to 3
- slot_row: int32 [4, 8, 32], P('grp', 'ep'), may hold values from 0 to 31
- block_count: int32 [4, 8, 8], P('grp', 'ep'), may hold values from 0 to 4, as said below
Outputs:
- mixed: bfloat16 [1024, 4096], P(('grp', 'ep'))
The draws below stay inside these ranges and needn't reach their ends.
Inputs may be any that keep to these rules, and one draw needn't show every extreme that they name: `block_count`: every device's expert has at least one block with all 4 slots live.
All inputs are finite; a program needn't handle non-finite values.
Results may differ from the reference program's by a relative error of at most 0.009.
Values may be sent and summed in bfloat16 or wider, within the bound.
A program may use at most 64 MiB of HBM per device.

```python
import math
import jax
import jax.numpy as jnp
from jax import lax

D = 4096
FFW = 1024
TOK_DEV = 32
SEND = 4
EXPERTS = 8
GROUPS = 4
COLUMNS = 8
SLOTS = 32
TOKENS = 1024
N_EP = 8


def draw_block_count(key, part):
    base = jax.random.randint(jax.random.fold_in(key, 11), (GROUPS, EXPERTS, COLUMNS), 0, SEND + 1)
    chosen = jax.random.randint(jax.random.fold_in(key, 12), (GROUPS, EXPERTS, 1), 0, COLUMNS)
    places = jnp.arange(COLUMNS).astype(jnp.int32)[None, None, :]
    return jnp.where(places == chosen, SEND, base).astype(jnp.int32)


def place_ends(result, stream_key, smallest, top_value):
    index_at = [jax.random.randint(jax.random.fold_in(stream_key, axis), (), 0, length) for axis, length in enumerate(result.shape)]
    widest = result.shape.index(max(result.shape))
    neighbour = index_at[:widest] + [(index_at[widest] + 1) % result.shape[widest]] + index_at[widest + 1:]
    return result.at[tuple(index_at)].set(smallest).at[tuple(neighbour)].set(top_value)


def shard_levels(rng, extent, pieces, smallest, high):
    def one(dim, shards_of):
        draws = jax.random.uniform(jax.random.fold_in(jax.random.fold_in(rng, 6), dim), (shards_of,), jnp.float32, smallest / len(pieces), high / len(pieces))
        return jnp.repeat(jnp.exp(draws), extent[dim] // shards_of).reshape((-1,) + (1,) * (len(extent) - dim - 1))

    gain = one(*pieces[0])
    for cut in pieces[1:]:
        gain = gain * one(*cut)
    return gain


def normal_values(rng, extent, width, bound, pieces=(), dtype=jnp.bfloat16):
    factor_of = shard_levels(rng, extent, pieces, -0.22, 0.18) if pieces else 1.0
    result = jax.random.normal(rng, extent, jnp.float32) * width * factor_of
    return jnp.minimum(jnp.maximum(result, -bound), bound).astype(dtype)


def setup_inputs(seed: int = 0) -> dict:
    key_of = jax.random.split(jax.random.key(seed), 7)
    hidden = normal_values(key_of[0], (GROUPS, EXPERTS, SLOTS, FFW), 1.0, 6.0, ((0, 4), (1, 8)))
    down_weight = normal_values(key_of[1], (EXPERTS, FFW, D), FFW ** -0.5, 0.1875, ((0, 8),))
    slot_gate = jnp.clip(jnp.exp(math.log(0.6) - 3.4011974 * jax.random.uniform(key_of[2], (GROUPS, EXPERTS, SLOTS), jnp.float32) ** shard_levels(key_of[2], (GROUPS, EXPERTS, SLOTS), ((0, 4), (1, 8)), -0.2, 0.2)), 0.02, 0.6)
    slot_owner = place_ends(jax.random.randint(key_of[3], (GROUPS, EXPERTS, SLOTS), 0, GROUPS), jax.random.fold_in(key_of[3], 1), 0, GROUPS - 1).astype(jnp.int32)
    slot_row = place_ends(jax.random.randint(key_of[4], (GROUPS, EXPERTS, SLOTS), 0, TOK_DEV), jax.random.fold_in(key_of[4], 1), 0, TOK_DEV - 1).astype(jnp.int32)
    block_count = draw_block_count(jax.random.fold_in(key_of[6], 71), 0)
    return {"hidden": hidden, "down_weight": down_weight, "slot_gate": slot_gate, "slot_owner": slot_owner, "slot_row": slot_row, "block_count": block_count}


def reference(hidden, down_weight, slot_gate, slot_owner, slot_row, block_count):
    column = (jnp.arange(SLOTS) // SEND).astype(jnp.int32)
    within = (jnp.arange(SLOTS) % SEND).astype(jnp.int32)

    def expert_rows(pair):
        rows_in, weight = pair
        return jnp.dot(rows_in, weight, preferred_element_type=jnp.float32)

    def group_step(total, inputs):
        group_hidden, gates, owners, row_index, counts = inputs
        product = lax.map(expert_rows, (group_hidden, down_weight))
        live = (within[None, :] < counts[:, column]).astype(jnp.float32)
        scale = gates * live
        sent = (product * scale[:, :, None]).astype(jnp.bfloat16)
        token = ((owners * N_EP + column[None, :]) * TOK_DEV + row_index).astype(jnp.int32)
        summed = jax.ops.segment_sum(sent.reshape(-1, D).astype(jnp.float32), token.reshape(-1), num_segments=TOKENS)
        rounded = lax.optimization_barrier(summed.astype(jnp.bfloat16))
        return total + rounded.astype(jnp.float32), None

    start = jnp.zeros((TOKENS, D), jnp.float32)
    total, unused = lax.scan(group_step, start, (hidden, slot_gate, slot_owner, slot_row, block_count))
    return total.astype(jnp.bfloat16)
```

```python
import functools

import jax
import jax.numpy as jnp
from jax import lax
from jax.experimental import pallas as pl
from jax.experimental.pallas import tpu as pltpu
from jax.sharding import PartitionSpec as P

TOK_DEV = 32
LANES = 128
VMEM_ROOM = 48 * 1024 * 1024
MESH = pl.DeviceIdType.MESH


def exchange_body(hidden, down_weight, slot_gate, slot_owner, slot_row, block_count):
    columns = lax.axis_size("ep")
    slot_total = hidden.shape[2]
    send = slot_total // columns
    product = jnp.dot(hidden[0, 0], down_weight[0], preferred_element_type=jnp.float32)
    within = jnp.arange(slot_total) % send
    limits = jnp.repeat(block_count[0, 0], send)
    live = (within < limits).astype(jnp.float32)
    scaled = (product * (slot_gate[0, 0] * live)[:, None]).astype(jnp.bfloat16)
    local_index = slot_owner[0, 0] * TOK_DEV + slot_row[0, 0]
    arrived, arrived_index = (
        lax.all_to_all(scaled, "ep", split_axis=0, concat_axis=0, tiled=True),
        lax.all_to_all(local_index, "ep", split_axis=0, concat_axis=0, tiled=True),
    )
    wanted = jnp.arange(lax.axis_size("grp") * TOK_DEV)
    table = (wanted[:, None] == arrived_index[None, :]).astype(jnp.bfloat16)
    return lax.psum_scatter(
        jnp.dot(table, arrived, preferred_element_type=jnp.float32).astype(jnp.bfloat16),
        "grp",
        scatter_dimension=0,
        tiled=True,
    )


def partner(me, n, k):
    if n & (n - 1):
        return lax.rem(me + n - k, n), lax.rem(me + k, n)
    other, bit = 0, 1
    while bit < n:
        mine = lax.rem(me // bit, 2)
        other = other + bit * (1 - mine if k & bit else mine)
        bit *= 2
    return other, other


def source_at(group, groups, step):
    if step == 0:
        return group
    if step == 1:
        return group + 1 - 2 * lax.rem(group, 2)
    lower = group < groups // 2
    place = jnp.where(lower, group, groups - 1 - group)
    base = place - lax.rem(place, 2)
    at = jnp.where(base > step - 2, step - 2, step)
    return jnp.where(lower, at, groups - 1 - at)


def kernel(
    groups, columns, send, piece,
    hidden_ref, weight_ref, gate_ref, owner_ref, row_ref, count_ref,
    sums, last_rows, last_table,
    gate, owner, row, count, weight, rows_in, meta, outgoing, arrived, places,
    load_sem, weight_sem, ready, hid_send, hid_recv, meta_send, meta_recv,
    row_send, row_recv, place_send, place_recv,
):
    group, column = lax.axis_index("grp"), lax.axis_index("ep")
    slots, width = hidden_ref.shape[2], weight_ref.shape[2]
    pieces = width // piece
    last = groups - 1
    batches = [2 if k == 0 and pieces % 2 == 0 else pieces for k in range(groups)]
    sources = [source_at(group, groups, k) for k in range(groups)]
    column_steps = sorted(range(1, columns), key=lambda k: (k % 2, -k)) if columns > 1 else []

    def weight_copy(j):
        cols = pl.ds(j * piece, piece)
        return pltpu.make_async_copy(
            weight_ref.at[0, :, cols], weight.at[:, cols], weight_sem.at[j]
        )

    barrier = pltpu.get_barrier_semaphore()
    for k in column_steps:
        pl.semaphore_signal(
            barrier, inc=1, device_id=(group, partner(column, columns, k)[0]), device_id_type=MESH
        )
    for t in range(groups):

        @pl.when((t > group) | (t == group - 1))
        def greet():
            pl.semaphore_signal(barrier, inc=1, device_id=(t, column), device_id_type=MESH)

    loads = [
        pltpu.make_async_copy(hidden_ref.at[0, 0], rows_in.at[group], load_sem.at[4]),
        pltpu.make_async_copy(gate_ref.at[0], gate, load_sem.at[0]),
        pltpu.make_async_copy(owner_ref.at[0], owner, load_sem.at[1]),
        pltpu.make_async_copy(row_ref.at[0], row, load_sem.at[2]),
        pltpu.make_async_copy(count_ref.at[0], count, load_sem.at[3]),
    ]
    for load in loads:
        load.start()
    for j in range(pieces):
        weight_copy(j).start()

    for load in loads:
        load.wait()
    lane = lax.broadcasted_iota(jnp.int32, (1, slots), 1)
    limit = jnp.zeros((1, slots), jnp.int32)
    for q in range(columns):
        limit = jnp.where(lane // send == q, count[:, q:q + 1], limit)
    scale = jnp.where(lane % send < limit, gate[...], 0.0)
    meta[group] = jnp.zeros(meta.shape[1:], jnp.float32)
    meta[group, 0, :, :slots] = scale
    meta[group, 1, :, :slots] = (owner[...] * TOK_DEV + row[...]).astype(jnp.float32)

    pl.semaphore_wait(barrier, columns - 1 + group + jnp.where(group < last, 1, 0))

    def hidden_copy(at, to):
        return pltpu.make_async_remote_copy(
            src_ref=rows_in.at[at], dst_ref=rows_in.at[at],
            send_sem=hid_send.at[to], recv_sem=hid_recv.at[at],
            device_id=(to, column), device_id_type=MESH,
        )

    def meta_copy(at, to):
        return pltpu.make_async_remote_copy(
            src_ref=meta.at[at], dst_ref=meta.at[at],
            send_sem=meta_send.at[to], recv_sem=meta_recv.at[at],
            device_id=(to, column), device_id_type=MESH,
        )

    def rows_at(k):
        return last_rows if k == last else arrived.at[k]

    def row_copy(k, m, j):
        to = partner(column, columns, m)[0]
        cols = pl.ds(j * piece, batches[k] * piece)
        return pltpu.make_async_remote_copy(
            src_ref=outgoing.at[k, to, :, cols], dst_ref=rows_at(k).at[column, :, cols],
            send_sem=row_send.at[k], recv_sem=row_recv.at[k],
            device_id=(group, to), device_id_type=MESH,
        )

    def place_copy(m):
        return pltpu.make_async_remote_copy(
            src_ref=meta.at[:, 1], dst_ref=places.at[column],
            send_sem=place_send, recv_sem=place_recv,
            device_id=(group, partner(column, columns, m)[0]), device_id_type=MESH,
        )

    def all_rows(k):
        return pltpu.make_async_remote_copy(
            src_ref=outgoing.at[k, pl.ds(0, columns - 1)],
            dst_ref=rows_at(k).at[pl.ds(0, columns - 1)],
            send_sem=row_send.at[k], recv_sem=row_recv.at[k],
            device_id=(group, partner(column, columns, 1)[0]), device_id_type=MESH,
        )

    def all_places():
        return pltpu.make_async_remote_copy(
            src_ref=places.at[pl.ds(0, columns - 1)],
            dst_ref=places.at[pl.ds(0, columns - 1)],
            send_sem=place_send, recv_sem=place_recv,
            device_id=(group, partner(column, columns, 1)[0]), device_id_type=MESH,
        )

    def share(to):
        meta_copy(group, to).start()
        hidden_copy(group, to).start()

    if groups > 1:
        share(sources[1])
    for t in range(groups):

        @pl.when((t < group) & (t != sources[min(1, groups - 1)]) | (t == group + 1) & (lax.rem(group, 2) == 1))
        def share_near():
            share(t)

        @pl.when(t < group - 1)
        def say_ready():
            pl.semaphore_signal(
                ready.at[group], inc=1, device_id=(t, column), device_id_type=MESH
            )

    def share_far(to):
        @pl.when(to < groups)
        def wait_and_share():
            pl.semaphore_wait(ready.at[to], 1)
            share(to)

    eye = lax.broadcasted_iota(jnp.int32, (slots, slots), 0) == lax.broadcasted_iota(
        jnp.int32, (slots, slots), 1
    )
    for k in range(groups):
        if k:
            meta_copy(sources[k], sources[k]).wait_recv()
            hidden_copy(sources[k], sources[k]).wait_recv()
        if k == last:
            for m in column_steps:
                place_copy(m).start()
            places[column] = meta[:, 1]
        factor = jnp.sum(jnp.where(eye, meta[sources[k], 0, :, :slots], 0.0), axis=1, keepdims=True)
        for j in range(pieces):
            if k == 0:
                weight_copy(j).wait()
            cols = slice(j * piece, (j + 1) * piece)
            product = jnp.dot(rows_in[sources[k]], weight[:, cols], preferred_element_type=jnp.float32)
            scaled = product * factor
            for q in range(columns):
                outgoing[k, q, :, cols] = scaled[q * send:(q + 1) * send].astype(jnp.bfloat16)
            if (j + 1) % batches[k] == 0:
                for m in column_steps:
                    row_copy(k, m, j + 1 - batches[k]).start()
        rows_at(k)[column] = outgoing[k, column]
        share_far(group + 2 + k)

    total = columns * send
    lanes = meta.shape[3]
    picked = lax.broadcasted_iota(jnp.int32, (lanes, total), 0) == (
        column * send + lax.broadcasted_iota(jnp.int32, (lanes, total), 1) % send
    )
    picked = picked.astype(jnp.float32)
    mine = lax.broadcasted_iota(jnp.int32, (columns, total), 0) == (
        lax.broadcasted_iota(jnp.int32, (columns, total), 1) // send
    )
    wanted = (
        group * TOK_DEV + lax.broadcasted_iota(jnp.int32, (TOK_DEV, total), 0)
    ).astype(jnp.float32)
    if column_steps:
        all_places().wait_recv()
    tables = []
    for k in range(groups):
        index = jnp.dot(
            places[:, sources[k], 0], picked,
            precision=lax.Precision.HIGHEST, preferred_element_type=jnp.float32,
        )
        index = jnp.sum(jnp.where(mine, index, 0.0), axis=0, keepdims=True)
        tables.append((wanted == index).astype(jnp.bfloat16))
    last_table[...] = tables[last]
    for k in range(last):
        if column_steps:
            all_rows(k).wait_recv()
        for j in range(pieces):
            cols = slice(j * piece, (j + 1) * piece)
            block = jnp.concatenate([arrived[k, e, :, cols] for e in range(columns)], axis=0)
            rows = jnp.dot(tables[k], block, preferred_element_type=jnp.float32)
            sums[:, cols] = sums[:, cols] + rows if k else rows
    if not last:
        sums[...] = jnp.zeros(sums.shape, jnp.float32)

    for k in range(1, groups):
        meta_copy(group, sources[k]).wait_send()
        hidden_copy(group, sources[k]).wait_send()
    if column_steps:
        all_places().wait_send()
        for k in range(groups):
            all_rows(k).wait_send()
        all_rows(last).wait_recv()


def finish(piece, sums, last_rows, last_table, out_ref, result, store_sem):
    columns, width = last_rows.shape[0], last_rows.shape[2]
    copies = []
    for j in range(width // piece):
        cols = slice(j * piece, (j + 1) * piece)
        block = jnp.concatenate([last_rows[e, :, cols] for e in range(columns)], axis=0)
        rows = jnp.dot(last_table[...], block, preferred_element_type=jnp.float32)
        result[:, cols] = (sums[:, cols] + rows).astype(out_ref.dtype)
        copy = pltpu.make_async_copy(
            result.at[:, cols], out_ref.at[:, cols], store_sem.at[j]
        )
        copy.start()
        copies.append(copy)
    for copy in copies:
        copy.wait()


def kernel_body(hidden, down_weight, slot_gate, slot_owner, slot_row, block_count):
    groups, columns = lax.axis_size("grp"), lax.axis_size("ep")
    slots, depth = hidden.shape[2:]
    width = down_weight.shape[2]
    send = slots // columns
    lanes = -(-slots // LANES) * LANES
    piece = 1024 if width % 1024 == 0 else width
    pieces = width // piece
    hbm = pl.BlockSpec(memory_space=pltpu.HBM)
    vmem = pl.BlockSpec(memory_space=pltpu.VMEM)
    dma = pltpu.SemaphoreType.DMA
    held = pl.pallas_call(
        functools.partial(kernel, groups, columns, send, piece),
        out_shape=(
            pltpu.VMEM((TOK_DEV, width), jnp.float32),
            pltpu.VMEM((columns, send, width), jnp.bfloat16),
            pltpu.VMEM((TOK_DEV, columns * send), jnp.bfloat16),
        ),
        in_specs=[hbm] * 6,
        out_specs=(vmem,) * 3,
        scratch_shapes=[
            pltpu.VMEM((1, slots), jnp.float32),
            pltpu.VMEM((1, slots), jnp.int32),
            pltpu.VMEM((1, slots), jnp.int32),
            pltpu.VMEM((1, columns), jnp.int32),
            pltpu.VMEM((depth, width), jnp.bfloat16),
            pltpu.VMEM((groups, slots, depth), jnp.bfloat16),
            pltpu.VMEM((groups, 2, 1, lanes), jnp.float32),
            pltpu.VMEM((groups, columns, send, width), jnp.bfloat16),
            pltpu.VMEM((max(groups - 1, 1), columns, send, width), jnp.bfloat16),
            pltpu.VMEM((columns, groups, 1, lanes), jnp.float32),
            dma((5,)), dma((pieces,)), pltpu.SemaphoreType.REGULAR((groups,)),
            dma((groups,)), dma((groups,)), dma((groups,)), dma((groups,)),
            dma((groups,)), dma((groups,)), dma, dma,
        ],
        compiler_params=pltpu.CompilerParams(
            collective_id=0, has_side_effects=True, vmem_limit_bytes=60 * 1024 * 1024
        ),
    )(hidden, down_weight, slot_gate, slot_owner, slot_row, block_count)
    return pl.pallas_call(
        functools.partial(finish, piece),
        out_shape=jax.ShapeDtypeStruct((TOK_DEV, width), jnp.bfloat16),
        in_specs=[vmem] * 3,
        out_specs=hbm,
        scratch_shapes=[pltpu.VMEM((TOK_DEV, width), jnp.bfloat16), dma((pieces,))],
        compiler_params=pltpu.CompilerParams(vmem_limit_bytes=8 * 1024 * 1024),
    )(*held)


def body(hidden, down_weight, *slot_data):
    groups, columns = lax.axis_size("grp"), lax.axis_size("ep")
    slots, depth = hidden.shape[2:]
    width = down_weight.shape[2]
    held = 2 * (depth * width + groups * slots * (depth + 2 * width))
    fits = held <= VMEM_ROOM and groups % 2 == 0
    chosen = kernel_body if fits else exchange_body
    return chosen(hidden, down_weight, *slot_data)


def solution(mesh):
    in_specs = (
        P("grp", "ep", None, None),
        P("ep", None, None),
        P("grp", "ep", None),
        P("grp", "ep", None),
        P("grp", "ep", None),
        P("grp", "ep", None),
    )
    out_specs = P(("grp", "ep"), None)
    return jax.shard_map(body, mesh=mesh, in_specs=in_specs, out_specs=out_specs, check_vma=False)
```

```python
import functools

import jax
import jax.numpy as jnp
from jax import lax
from jax.experimental import pallas as pl
from jax.experimental.pallas import tpu as pltpu
from jax.sharding import PartitionSpec as P

TOK_DEV = 32
LANES = 128
PIECE = 1024
PLANES = 4
VMEM_ROOM = 48 * 1024 * 1024
MESH = pl.DeviceIdType.MESH


def exchange_body(hidden, down_weight, slot_gate, slot_owner, slot_row, block_count):
    columns = lax.axis_size("ep")
    slot_total = hidden.shape[2]
    send = slot_total // columns
    product = jnp.dot(hidden[0, 0], down_weight[0], preferred_element_type=jnp.float32)
    within = jnp.arange(slot_total) % send
    limits = jnp.repeat(block_count[0, 0], send)
    live = (within < limits).astype(jnp.float32)
    scaled = (product * (slot_gate[0, 0] * live)[:, None]).astype(jnp.bfloat16)
    local_index = slot_owner[0, 0] * TOK_DEV + slot_row[0, 0]
    arrived, arrived_index = (
        lax.all_to_all(scaled, "ep", split_axis=0, concat_axis=0, tiled=True),
        lax.all_to_all(local_index, "ep", split_axis=0, concat_axis=0, tiled=True),
    )
    wanted = jnp.arange(lax.axis_size("grp") * TOK_DEV)
    table = (wanted[:, None] == arrived_index[None, :]).astype(jnp.bfloat16)
    return lax.psum_scatter(
        jnp.dot(table, arrived, preferred_element_type=jnp.float32).astype(jnp.bfloat16),
        "grp",
        scatter_dimension=0,
        tiled=True,
    )


def partner(me, n, k):
    if n & (n - 1):
        return lax.rem(me + n - k, n), lax.rem(me + k, n)
    other, bit = 0, 1
    while bit < n:
        mine = lax.rem(me // bit, 2)
        other = other + bit * (1 - mine if k & bit else mine)
        bit *= 2
    return other, other


def local_cols(group, width, start, size):
    at = lax.rem(start + lax.rem(group, 2) * (width // 2), width)
    return pl.ds(pl.multiple_of(at, size), size)


def kernel(
    groups, columns, send, piece,
    hidden_ref, weight_ref, gate_ref, owner_ref, row_ref, count_ref,
    sums, last_rows, last_table,
    gate, owner, row, count, weight, rows_in, meta,
    out_early, out_late, in_early, in_late, pair_places, places, swap_out, swap_in,
    load_sem, weight_sem, hid_send, hid_recv, meta_send, meta_recv,
    row_send, row_recv, place_send, place_recv, swap_send, swap_recv,
):
    group, column = lax.axis_index("grp"), lax.axis_index("ep")
    slots, width = hidden_ref.shape[2], weight_ref.shape[2]
    half = width // 2
    last = groups - 1
    total = columns * send
    pair = group + 1 - 2 * lax.rem(group, 2)
    pair_base = group - lax.rem(group, 2)
    far, far_pair = last - group, last - pair
    end = group == last
    sources = [group, pair, jnp.where(end, far_pair, far), jnp.where(end, far, far_pair)]
    column_steps = sorted(range(1, columns), key=lambda k: (k % 2, -k))

    def weight_copy(j):
        return pltpu.make_async_copy(
            weight_ref.at[0, :, local_cols(group, width, j * piece, piece)],
            weight.at[:, pl.ds(j * piece, piece)],
            weight_sem.at[j],
        )

    loads = [
        pltpu.make_async_copy(hidden_ref.at[0, 0], rows_in.at[group], load_sem.at[4]),
        pltpu.make_async_copy(gate_ref.at[0], gate, load_sem.at[0]),
        pltpu.make_async_copy(owner_ref.at[0], owner, load_sem.at[1]),
        pltpu.make_async_copy(row_ref.at[0], row, load_sem.at[2]),
        pltpu.make_async_copy(count_ref.at[0], count, load_sem.at[3]),
    ]
    for load in loads:
        load.start()

    barrier = pltpu.get_barrier_semaphore()
    for k in column_steps:
        pl.semaphore_signal(
            barrier, inc=1, device_id=(group, partner(column, columns, k)[0]), device_id_type=MESH
        )
    pl.semaphore_signal(barrier, inc=1, device_id=(pair, column), device_id_type=MESH)

    @pl.when(group < last)
    def greet_far():
        pl.semaphore_signal(barrier, inc=1, device_id=(far, column), device_id_type=MESH)

    for load in loads:
        load.wait()
    for j in range(width // piece):
        weight_copy(j).start()
    lane = lax.broadcasted_iota(jnp.int32, (1, slots), 1)
    limit = jnp.zeros((1, slots), jnp.int32)
    for q in range(columns):
        limit = jnp.where(lane // send == q, count[:, q:q + 1], limit)
    scale = jnp.where(lane % send < limit, gate[...], 0.0)
    meta[group] = jnp.zeros(meta.shape[1:], jnp.float32)
    meta[group, 0, :, :slots] = scale
    meta[group, 1, :, :slots] = (owner[...] * TOK_DEV + row[...]).astype(jnp.float32)

    pl.semaphore_wait(barrier, columns + jnp.where(group > 0, 1, 0))

    def share_copies(at, to, slot=None):
        slot = at if slot is None else slot
        return [
            pltpu.make_async_remote_copy(
                src_ref=held.at[at], dst_ref=held.at[at],
                send_sem=sent.at[slot], recv_sem=landed.at[at],
                device_id=(to, column), device_id_type=MESH,
            )
            for held, sent, landed in ((meta, meta_send, meta_recv), (rows_in, hid_send, hid_recv))
        ]

    def share(at, to, slot=None):
        for copy in share_copies(at, to, slot):
            copy.start()

    def wait_shared(at):
        for copy in share_copies(at, at):
            copy.wait_recv()

    def wait_sent(slot):
        for copy in share_copies(group, pair, slot):
            copy.wait_send()

    def rows_out(k):
        return out_early.at[k] if k < 2 else out_late.at[k - 2]

    def rows_at(k):
        return in_early.at[k] if k < 2 else last_rows if k == last else in_late.at[k - 2]

    def row_copy(k, m, j, batch):
        to = partner(column, columns, m)[0]
        cols = pl.ds(j * piece, batch * piece)
        return pltpu.make_async_remote_copy(
            src_ref=rows_out(k).at[to, :, cols], dst_ref=rows_at(k).at[column, :, cols],
            send_sem=row_send.at[k], recv_sem=row_recv.at[k],
            device_id=(group, to), device_id_type=MESH,
        )

    def all_rows(k):
        return pltpu.make_async_remote_copy(
            src_ref=rows_out(k).at[pl.ds(0, columns - 1)],
            dst_ref=rows_at(k).at[pl.ds(0, columns - 1)],
            send_sem=row_send.at[k], recv_sem=row_recv.at[k],
            device_id=(group, partner(column, columns, 1)[0]), device_id_type=MESH,
        )

    def place_copy(k, m):
        src = meta.at[sources[k], 1] if k > 1 else meta.at[pl.ds(pair_base, 2), 1]
        dst = places.at[k - 2, column] if k > 1 else pair_places.at[column]
        return pltpu.make_async_remote_copy(
            src_ref=src, dst_ref=dst,
            send_sem=place_send.at[k - 1], recv_sem=place_recv.at[k - 1],
            device_id=(group, partner(column, columns, m)[0]), device_id_type=MESH,
        )

    def all_places(k):
        some = (places.at[k - 2] if k > 1 else pair_places).at[pl.ds(0, columns - 1)]
        return pltpu.make_async_remote_copy(
            src_ref=some, dst_ref=some,
            send_sem=place_send.at[k - 1], recv_sem=place_recv.at[k - 1],
            device_id=(group, partner(column, columns, 1)[0]), device_id_type=MESH,
        )

    def swap_copy(j):
        cols = pl.ds(j * piece, piece)
        return pltpu.make_async_remote_copy(
            src_ref=swap_out.at[:, cols], dst_ref=swap_in.at[:, cols],
            send_sem=swap_send.at[j], recv_sem=swap_recv.at[j],
            device_id=(pair, column), device_id_type=MESH,
        )

    share(group, pair)

    @pl.when(group > 0)
    def share_far():
        share(group, far, groups)

    eye = lax.broadcasted_iota(jnp.int32, (slots, slots), 0) == lax.broadcasted_iota(
        jnp.int32, (slots, slots), 1
    )
    lanes = meta.shape[3]
    picked = lax.broadcasted_iota(jnp.int32, (lanes, total), 0) == (
        column * send + lax.broadcasted_iota(jnp.int32, (lanes, total), 1) % send
    )
    picked = picked.astype(jnp.float32)
    mine = lax.broadcasted_iota(jnp.int32, (columns, total), 0) == (
        lax.broadcasted_iota(jnp.int32, (columns, total), 1) // send
    )
    token = lax.broadcasted_iota(jnp.int32, (TOK_DEV, total), 0)

    def table_of(found, owners):
        index = jnp.dot(
            found, picked, precision=lax.Precision.HIGHEST, preferred_element_type=jnp.float32
        )
        index = jnp.sum(jnp.where(mine, index, 0.0), axis=0, keepdims=True)
        return [
            ((owner_group * TOK_DEV + token).astype(jnp.float32) == index).astype(jnp.bfloat16)
            for owner_group in owners
        ]

    def block(k, cols):
        return jnp.concatenate([rows_at(k)[e, :, cols] for e in range(columns)], axis=0)

    def early_sums():
        all_places(1).wait_recv()
        both = []
        for k in range(2):
            found = pair_places[:, sources[k] - pair_base, 0]
            both.append(jnp.concatenate(table_of(found, (group, pair)), axis=0))
        table = jnp.concatenate(both, axis=1)
        for k in range(2):
            all_rows(k).wait_recv()
        for j in range(half // piece):
            cols = slice(j * piece, (j + 1) * piece)
            rows = jnp.concatenate([block(0, cols), block(1, cols)], axis=0)
            rows = jnp.dot(table, rows, preferred_element_type=jnp.float32)
            swap_out[:, cols] = rows[TOK_DEV:].astype(jnp.bfloat16)
            swap_copy(j).start()
            sums[:, cols] = rows[:TOK_DEV]

    for k in range(groups):
        if k in (1, 2):
            wait_shared(sources[k])

            @pl.when(group == 1 if k == 1 else group < last)
            def forward():
                share(sources[k], far if k == 1 else pair)

        if k == last:

            @pl.when(group != last - 1)
            def wait_last():
                wait_shared(sources[k])

        if k:
            for m in column_steps:
                place_copy(k, m).start()
        if k == 1:
            pair_places[column] = meta[pl.ds(pair_base, 2), 1]
        elif k > 1:
            places[k - 2, column] = meta[sources[k], 1]
        factor = jnp.sum(jnp.where(eye, meta[sources[k], 0, :, :slots], 0.0), axis=1, keepdims=True)
        batch = 1
        for j in range((half if k < 2 else width) // piece):
            if k == 0 or k == 2 and j >= half // piece:
                weight_copy(j).wait()
            cols = slice(j * piece, (j + 1) * piece)
            product = jnp.dot(rows_in[sources[k]], weight[:, cols], preferred_element_type=jnp.float32)
            scaled = product * factor
            for q in range(columns):
                rows_out(k)[q, :, cols] = scaled[q * send:(q + 1) * send].astype(jnp.bfloat16)
            if (j + 1) % batch == 0:
                for m in column_steps:
                    row_copy(k, m, j + 1 - batch, batch).start()
        rows_at(k)[column] = rows_out(k)[column]
        if k == 2:

            @pl.when(group == last - 1)
            def forward_last():
                wait_shared(sources[last])
                share(sources[last], pair)

            early_sums()

    tables = []
    for k in range(2, groups):
        all_places(k).wait_recv()
        tables.append(table_of(places[k - 2, :, 0], (group,))[0])
    last_table[...] = tables[-1]
    for k in range(2, last):
        all_rows(k).wait_recv()
        if k == 2:
            for j in range(half // piece):
                swap_copy(j).wait_recv()
        for j in range(width // piece):
            cols = slice(j * piece, (j + 1) * piece)
            rows = jnp.dot(tables[k - 2], block(k, cols), preferred_element_type=jnp.float32)
            if k > 2 or j < half // piece:
                sums[:, cols] = sums[:, cols] + rows
            else:
                swapped = swap_in[:, j * piece - half:(j + 1) * piece - half]
                sums[:, cols] = swapped.astype(jnp.float32) + rows

    wait_sent(group)

    @pl.when(group > 0)
    def sent_far():
        wait_sent(groups)

    @pl.when(group == 1)
    def sent_first():
        wait_sent(sources[1])

    @pl.when(group < last)
    def sent_second():
        wait_sent(sources[2])

    @pl.when(group == last - 1)
    def sent_last():
        wait_sent(sources[last])

    for k in range(1, groups):
        all_places(k).wait_send()
    for j in range(half // piece):
        swap_copy(j).wait_send()
    all_rows(last).wait_recv()
    for k in range(groups):
        all_rows(k).wait_send()


def finish(piece, sums, last_rows, last_table, out_ref, result, store_sem):
    group = lax.axis_index("grp")
    columns, width = last_rows.shape[0], last_rows.shape[2]
    copies = []
    for j in range(width // piece):
        cols = slice(j * piece, (j + 1) * piece)
        block = jnp.concatenate([last_rows[e, :, cols] for e in range(columns)], axis=0)
        rows = jnp.dot(last_table[...], block, preferred_element_type=jnp.float32)
        result[:, cols] = (sums[:, cols] + rows).astype(out_ref.dtype)
        copy = pltpu.make_async_copy(
            result.at[:, cols],
            out_ref.at[:, local_cols(group, width, j * piece, piece)],
            store_sem.at[j],
        )
        copy.start()
        copies.append(copy)
    for copy in copies:
        copy.wait()


def kernel_body(hidden, down_weight, slot_gate, slot_owner, slot_row, block_count):
    groups, columns = lax.axis_size("grp"), lax.axis_size("ep")
    slots, depth = hidden.shape[2:]
    width = down_weight.shape[2]
    send = slots // columns
    lanes = -(-slots // LANES) * LANES
    pieces, halves = width // PIECE, width // 2 // PIECE
    hbm = pl.BlockSpec(memory_space=pltpu.HBM)
    vmem = pl.BlockSpec(memory_space=pltpu.VMEM)
    dma = pltpu.SemaphoreType.DMA
    held = pl.pallas_call(
        functools.partial(kernel, groups, columns, send, PIECE),
        out_shape=(
            pltpu.VMEM((TOK_DEV, width), jnp.float32),
            pltpu.VMEM((columns, send, width), jnp.bfloat16),
            pltpu.VMEM((TOK_DEV, columns * send), jnp.bfloat16),
        ),
        in_specs=[hbm] * 6,
        out_specs=(vmem,) * 3,
        scratch_shapes=[
            pltpu.VMEM((1, slots), jnp.float32),
            pltpu.VMEM((1, slots), jnp.int32),
            pltpu.VMEM((1, slots), jnp.int32),
            pltpu.VMEM((1, columns), jnp.int32),
            pltpu.VMEM((depth, width), jnp.bfloat16),
            pltpu.VMEM((groups, slots, depth), jnp.bfloat16),
            pltpu.VMEM((groups, 2, 1, lanes), jnp.float32),
            pltpu.VMEM((2, columns, send, width // 2), jnp.bfloat16),
            pltpu.VMEM((groups - 2, columns, send, width), jnp.bfloat16),
            pltpu.VMEM((2, columns, send, width // 2), jnp.bfloat16),
            pltpu.VMEM((groups - 3, columns, send, width), jnp.bfloat16),
            pltpu.VMEM((columns, 2, 1, lanes), jnp.float32),
            pltpu.VMEM((groups - 2, columns, 1, lanes), jnp.float32),
            pltpu.VMEM((TOK_DEV, width // 2), jnp.bfloat16),
            pltpu.VMEM((TOK_DEV, width // 2), jnp.bfloat16),
            dma((5,)), dma((pieces,)),
            dma((groups + 1,)), dma((groups,)), dma((groups + 1,)), dma((groups,)),
            dma((groups,)), dma((groups,)), dma((groups - 1,)), dma((groups - 1,)),
            dma((halves,)), dma((halves,)),
        ],
        compiler_params=pltpu.CompilerParams(
            collective_id=0, has_side_effects=True, vmem_limit_bytes=60 * 1024 * 1024
        ),
    )(hidden, down_weight, slot_gate, slot_owner, slot_row, block_count)
    return pl.pallas_call(
        functools.partial(finish, PIECE),
        out_shape=jax.ShapeDtypeStruct((TOK_DEV, width), jnp.bfloat16),
        in_specs=[vmem] * 3,
        out_specs=hbm,
        scratch_shapes=[pltpu.VMEM((TOK_DEV, width), jnp.bfloat16), dma((pieces,))],
        compiler_params=pltpu.CompilerParams(vmem_limit_bytes=8 * 1024 * 1024),
    )(*held)


def body(hidden, down_weight, *slot_data):
    groups, columns = lax.axis_size("grp"), lax.axis_size("ep")
    slots, depth = hidden.shape[2:]
    width = down_weight.shape[2]
    held = 2 * (depth * width + groups * slots * (depth + 2 * width))
    even = groups == PLANES and columns > 1 and width % (2 * PIECE) == 0
    fits = held <= VMEM_ROOM and even
    chosen = kernel_body if fits else exchange_body
    return chosen(hidden, down_weight, *slot_data)


def solution(mesh):
    in_specs = (
        P("grp", "ep", None, None),
        P("ep", None, None),
        P("grp", "ep", None),
        P("grp", "ep", None),
        P("grp", "ep", None),
        P("grp", "ep", None),
    )
    out_specs = P(("grp", "ep"), None)
    return jax.shard_map(body, mesh=mesh, in_specs=in_specs, out_specs=out_specs, check_vma=False)
```

```python
import functools

import jax
import jax.numpy as jnp
from jax import lax
from jax.experimental import pallas as pl
from jax.experimental.pallas import tpu as pltpu
from jax.sharding import PartitionSpec as P

TOK_DEV = 32
LANES = 128
PIECE = 1024
PLANES = 4
VMEM_ROOM = 48 * 1024 * 1024
MESH = pl.DeviceIdType.MESH


def exchange_body(hidden, down_weight, slot_gate, slot_owner, slot_row, block_count):
    columns = lax.axis_size("ep")
    slot_total = hidden.shape[2]
    send = slot_total // columns
    product = jnp.dot(hidden[0, 0], down_weight[0], preferred_element_type=jnp.float32)
    within = jnp.arange(slot_total) % send
    limits = jnp.repeat(block_count[0, 0], send)
    live = (within < limits).astype(jnp.float32)
    scaled = (product * (slot_gate[0, 0] * live)[:, None]).astype(jnp.bfloat16)
    local_index = slot_owner[0, 0] * TOK_DEV + slot_row[0, 0]
    arrived, arrived_index = (
        lax.all_to_all(scaled, "ep", split_axis=0, concat_axis=0, tiled=True),
        lax.all_to_all(local_index, "ep", split_axis=0, concat_axis=0, tiled=True),
    )
    wanted = jnp.arange(lax.axis_size("grp") * TOK_DEV)
    table = (wanted[:, None] == arrived_index[None, :]).astype(jnp.bfloat16)
    return lax.psum_scatter(
        jnp.dot(table, arrived, preferred_element_type=jnp.float32).astype(jnp.bfloat16),
        "grp",
        scatter_dimension=0,
        tiled=True,
    )


def partner(me, n, k):
    if n & (n - 1):
        return lax.rem(me + n - k, n), lax.rem(me + k, n)
    other, bit = 0, 1
    while bit < n:
        mine = lax.rem(me // bit, 2)
        other = other + bit * (1 - mine if k & bit else mine)
        bit *= 2
    return other, other


def local_cols(group, width, start, size):
    at = lax.rem(start + lax.rem(group, 2) * (width // 2), width)
    return pl.ds(pl.multiple_of(at, size), size)


def kernel(
    groups, columns, send, piece,
    hidden_ref, weight_ref, gate_ref, owner_ref, row_ref, count_ref,
    sums, last_rows, last_table,
    gate, owner, row, count, weight, rows_in, meta,
    out_early, out_late, in_early, in_late, pair_places, places, swap_out, swap_in,
    load_sem, weight_sem, hid_send, hid_recv, meta_send, meta_recv,
    row_send, row_recv, place_send, place_recv, swap_send, swap_recv,
):
    group, column = lax.axis_index("grp"), lax.axis_index("ep")
    slots, width = hidden_ref.shape[2], weight_ref.shape[2]
    half = width // 2
    last = groups - 1
    total = columns * send
    pair = group + 1 - 2 * lax.rem(group, 2)
    pair_base = group - lax.rem(group, 2)
    far, far_pair = last - group, last - pair
    end = group == last
    sources = [group, pair, jnp.where(end, far_pair, far), jnp.where(end, far, far_pair)]
    column_steps = sorted(range(1, columns), key=lambda k: (k % 2, -k))

    def weight_copy(j):
        return pltpu.make_async_copy(
            weight_ref.at[0, :, local_cols(group, width, j * piece, piece)],
            weight.at[:, pl.ds(j * piece, piece)],
            weight_sem.at[j],
        )

    loads = [
        pltpu.make_async_copy(hidden_ref.at[0, 0], rows_in.at[group], load_sem.at[4]),
        pltpu.make_async_copy(gate_ref.at[0], gate, load_sem.at[0]),
        pltpu.make_async_copy(owner_ref.at[0], owner, load_sem.at[1]),
        pltpu.make_async_copy(row_ref.at[0], row, load_sem.at[2]),
        pltpu.make_async_copy(count_ref.at[0], count, load_sem.at[3]),
    ]
    for load in loads:
        load.start()

    barrier = pltpu.get_barrier_semaphore()
    for k in column_steps:
        pl.semaphore_signal(
            barrier, inc=1, device_id=(group, partner(column, columns, k)[0]), device_id_type=MESH
        )
    pl.semaphore_signal(barrier, inc=1, device_id=(pair, column), device_id_type=MESH)

    @pl.when(group < last)
    def greet_far():
        pl.semaphore_signal(barrier, inc=1, device_id=(far, column), device_id_type=MESH)

    for load in loads:
        load.wait()
    for j in range(width // piece):
        weight_copy(j).start()
    lane = lax.broadcasted_iota(jnp.int32, (1, slots), 1)
    limit = jnp.zeros((1, slots), jnp.int32)
    for q in range(columns):
        limit = jnp.where(lane // send == q, count[:, q:q + 1], limit)
    scale = jnp.where(lane % send < limit, gate[...], 0.0)
    meta[group] = jnp.zeros(meta.shape[1:], jnp.float32)
    meta[group, 0, :, :slots] = scale
    meta[group, 1, :, :slots] = (owner[...] * TOK_DEV + row[...]).astype(jnp.float32)

    pl.semaphore_wait(barrier, columns + jnp.where(group > 0, 1, 0))

    def share_copies(at, to, slot=None):
        slot = at if slot is None else slot
        return [
            pltpu.make_async_remote_copy(
                src_ref=held.at[at], dst_ref=held.at[at],
                send_sem=sent.at[slot], recv_sem=landed.at[at],
                device_id=(to, column), device_id_type=MESH,
            )
            for held, sent, landed in ((meta, meta_send, meta_recv), (rows_in, hid_send, hid_recv))
        ]

    def share(at, to, slot=None):
        for copy in share_copies(at, to, slot):
            copy.start()

    def wait_shared(at):
        for copy in share_copies(at, at):
            copy.wait_recv()

    def wait_sent(slot):
        for copy in share_copies(group, pair, slot):
            copy.wait_send()

    def rows_out(k):
        return out_early.at[k] if k < 2 else out_late.at[k - 2]

    def rows_at(k):
        return in_early.at[k] if k < 2 else last_rows if k == last else in_late.at[k - 2]

    def row_copy(k, m, j, batch):
        to = partner(column, columns, m)[0]
        cols = pl.ds(j * piece, batch * piece)
        return pltpu.make_async_remote_copy(
            src_ref=rows_out(k).at[to, :, cols], dst_ref=rows_at(k).at[column, :, cols],
            send_sem=row_send.at[k], recv_sem=row_recv.at[k],
            device_id=(group, to), device_id_type=MESH,
        )

    def all_rows(k):
        return pltpu.make_async_remote_copy(
            src_ref=rows_out(k).at[pl.ds(0, columns - 1)],
            dst_ref=rows_at(k).at[pl.ds(0, columns - 1)],
            send_sem=row_send.at[k], recv_sem=row_recv.at[k],
            device_id=(group, partner(column, columns, 1)[0]), device_id_type=MESH,
        )

    def place_copy(k, m):
        src = meta.at[sources[k], 1] if k > 1 else meta.at[pl.ds(pair_base, 2), 1]
        dst = places.at[k - 2, column] if k > 1 else pair_places.at[column]
        return pltpu.make_async_remote_copy(
            src_ref=src, dst_ref=dst,
            send_sem=place_send.at[k - 1], recv_sem=place_recv.at[k - 1],
            device_id=(group, partner(column, columns, m)[0]), device_id_type=MESH,
        )

    def all_places(k):
        some = (places.at[k - 2] if k > 1 else pair_places).at[pl.ds(0, columns - 1)]
        return pltpu.make_async_remote_copy(
            src_ref=some, dst_ref=some,
            send_sem=place_send.at[k - 1], recv_sem=place_recv.at[k - 1],
            device_id=(group, partner(column, columns, 1)[0]), device_id_type=MESH,
        )

    def swap_copy(j):
        cols = pl.ds(j * piece, piece)
        return pltpu.make_async_remote_copy(
            src_ref=swap_out.at[:, cols], dst_ref=swap_in.at[:, cols],
            send_sem=swap_send.at[j], recv_sem=swap_recv.at[j],
            device_id=(pair, column), device_id_type=MESH,
        )

    @pl.when(group > 0)
    def share_far():
        share(group, far, groups)

    share(group, pair)
    eye = lax.broadcasted_iota(jnp.int32, (slots, slots), 0) == lax.broadcasted_iota(
        jnp.int32, (slots, slots), 1
    )
    lanes = meta.shape[3]
    picked = lax.broadcasted_iota(jnp.int32, (lanes, total), 0) == (
        column * send + lax.broadcasted_iota(jnp.int32, (lanes, total), 1) % send
    )
    picked = picked.astype(jnp.float32)
    mine = lax.broadcasted_iota(jnp.int32, (columns, total), 0) == (
        lax.broadcasted_iota(jnp.int32, (columns, total), 1) // send
    )
    token = lax.broadcasted_iota(jnp.int32, (TOK_DEV, total), 0)

    def table_of(found, owners):
        index = jnp.dot(
            found, picked, precision=lax.Precision.HIGHEST, preferred_element_type=jnp.float32
        )
        index = jnp.sum(jnp.where(mine, index, 0.0), axis=0, keepdims=True)
        return [
            ((owner_group * TOK_DEV + token).astype(jnp.float32) == index).astype(jnp.bfloat16)
            for owner_group in owners
        ]

    def block(k, cols):
        return jnp.concatenate([rows_at(k)[e, :, cols] for e in range(columns)], axis=0)

    def early_sums():
        all_places(1).wait_recv()
        both = []
        for k in range(2):
            found = pair_places[:, sources[k] - pair_base, 0]
            both.append(jnp.concatenate(table_of(found, (group, pair)), axis=0))
        table = jnp.concatenate(both, axis=1)
        for k in range(2):
            all_rows(k).wait_recv()
        for j in range(half // piece):
            cols = slice(j * piece, (j + 1) * piece)
            rows = jnp.concatenate([block(0, cols), block(1, cols)], axis=0)
            rows = jnp.dot(table, rows, preferred_element_type=jnp.float32)
            swap_out[:, cols] = rows[TOK_DEV:].astype(jnp.bfloat16)
            swap_copy(j).start()
            sums[:, cols] = rows[:TOK_DEV]

    def compute(k):
        factor = jnp.sum(jnp.where(eye, meta[sources[k], 0, :, :slots], 0.0), axis=1, keepdims=True)
        def product(j):
            if k == 0 or k == 2 and j >= half // piece:
                weight_copy(j).wait()
            cols = slice(j * piece, (j + 1) * piece)
            return jnp.dot(rows_in[sources[k]], weight[:, cols], preferred_element_type=jnp.float32)

        steps = (half if k < 2 else width) // piece
        ahead = product(0)
        for j in range(steps):
            scaled = ahead * factor
            if j + 1 < steps:
                ahead = product(j + 1)
            cols = slice(j * piece, (j + 1) * piece)
            for q in range(columns):
                rows_out(k)[q, :, cols] = scaled[q * send:(q + 1) * send].astype(jnp.bfloat16)
            for m in column_steps:
                row_copy(k, m, j, 1).start()
        rows_at(k)[column] = rows_out(k)[column]

    def take_pair():
        wait_shared(sources[1])

        @pl.when(group == 1)
        def forward_pair():
            share(sources[1], far)

        for m in column_steps:
            place_copy(1, m).start()
        pair_places[column] = meta[pl.ds(pair_base, 2), 1]
        compute(1)

    def take_third():
        wait_shared(sources[2])

        @pl.when(group < last)
        def forward_third():
            share(sources[2], pair)

        for m in column_steps:
            place_copy(2, m).start()
        places[0, column] = meta[sources[2], 1]
        compute(2)

    compute(0)

    @pl.when(group != last - 1)
    def pair_first():
        take_pair()
        take_third()

    @pl.when(group == last - 1)
    def third_first():
        take_third()
        wait_shared(sources[last])
        share(sources[last], pair)
        take_pair()

    @pl.when(lax.rem(group, 2) == 1)
    def early_first():
        early_sums()

    @pl.when(group != last - 1)
    def wait_last():
        wait_shared(sources[last])

    for m in column_steps:
        place_copy(last, m).start()
    places[last - 2, column] = meta[sources[last], 1]
    compute(last)

    @pl.when(lax.rem(group, 2) == 0)
    def early_after():
        early_sums()

    tables = []
    for k in range(2, groups):
        all_places(k).wait_recv()
        tables.append(table_of(places[k - 2, :, 0], (group,))[0])
    last_table[...] = tables[-1]
    for k in range(2, last):
        all_rows(k).wait_recv()
        if k == 2:
            for j in range(half // piece):
                swap_copy(j).wait_recv()
        for j in range(width // piece):
            cols = slice(j * piece, (j + 1) * piece)
            rows = jnp.dot(tables[k - 2], block(k, cols), preferred_element_type=jnp.float32)
            if k > 2 or j < half // piece:
                sums[:, cols] = sums[:, cols] + rows
            else:
                swapped = swap_in[:, j * piece - half:(j + 1) * piece - half]
                sums[:, cols] = swapped.astype(jnp.float32) + rows

    wait_sent(group)

    @pl.when(group > 0)
    def sent_far():
        wait_sent(groups)

    @pl.when(group == 1)
    def sent_first():
        wait_sent(sources[1])

    @pl.when(group < last)
    def sent_second():
        wait_sent(sources[2])

    @pl.when(group == last - 1)
    def sent_last():
        wait_sent(sources[last])

    for k in range(1, groups):
        all_places(k).wait_send()
    for j in range(half // piece):
        swap_copy(j).wait_send()
    all_rows(last).wait_recv()
    for k in range(groups):
        all_rows(k).wait_send()


def finish(piece, sums, last_rows, last_table, out_ref, result, store_sem):
    group = lax.axis_index("grp")
    columns, width = last_rows.shape[0], last_rows.shape[2]
    copies = []
    for j in range(width // piece):
        cols = slice(j * piece, (j + 1) * piece)
        block = jnp.concatenate([last_rows[e, :, cols] for e in range(columns)], axis=0)
        rows = jnp.dot(last_table[...], block, preferred_element_type=jnp.float32)
        result[:, cols] = (sums[:, cols] + rows).astype(out_ref.dtype)
        copy = pltpu.make_async_copy(
            result.at[:, cols],
            out_ref.at[:, local_cols(group, width, j * piece, piece)],
            store_sem.at[j],
        )
        copy.start()
        copies.append(copy)
    for copy in copies:
        copy.wait()


def kernel_body(hidden, down_weight, slot_gate, slot_owner, slot_row, block_count):
    groups, columns = lax.axis_size("grp"), lax.axis_size("ep")
    slots, depth = hidden.shape[2:]
    width = down_weight.shape[2]
    send = slots // columns
    lanes = -(-slots // LANES) * LANES
    pieces, halves = width // PIECE, width // 2 // PIECE
    hbm = pl.BlockSpec(memory_space=pltpu.HBM)
    vmem = pl.BlockSpec(memory_space=pltpu.VMEM)
    dma = pltpu.SemaphoreType.DMA
    held = pl.pallas_call(
        functools.partial(kernel, groups, columns, send, PIECE),
        out_shape=(
            pltpu.VMEM((TOK_DEV, width), jnp.float32),
            pltpu.VMEM((columns, send, width), jnp.bfloat16),
            pltpu.VMEM((TOK_DEV, columns * send), jnp.bfloat16),
        ),
        in_specs=[hbm] * 6,
        out_specs=(vmem,) * 3,
        scratch_shapes=[
            pltpu.VMEM((1, slots), jnp.float32),
            pltpu.VMEM((1, slots), jnp.int32),
            pltpu.VMEM((1, slots), jnp.int32),
            pltpu.VMEM((1, columns), jnp.int32),
            pltpu.VMEM((depth, width), jnp.bfloat16),
            pltpu.VMEM((groups, slots, depth), jnp.bfloat16),
            pltpu.VMEM((groups, 2, 1, lanes), jnp.float32),
            pltpu.VMEM((2, columns, send, width // 2), jnp.bfloat16),
            pltpu.VMEM((groups - 2, columns, send, width), jnp.bfloat16),
            pltpu.VMEM((2, columns, send, width // 2), jnp.bfloat16),
            pltpu.VMEM((groups - 3, columns, send, width), jnp.bfloat16),
            pltpu.VMEM((columns, 2, 1, lanes), jnp.float32),
            pltpu.VMEM((groups - 2, columns, 1, lanes), jnp.float32),
            pltpu.VMEM((TOK_DEV, width // 2), jnp.bfloat16),
            pltpu.VMEM((TOK_DEV, width // 2), jnp.bfloat16),
            dma((5,)), dma((pieces,)),
            dma((groups + 1,)), dma((groups,)), dma((groups + 1,)), dma((groups,)),
            dma((groups,)), dma((groups,)), dma((groups - 1,)), dma((groups - 1,)),
            dma((halves,)), dma((halves,)),
        ],
        compiler_params=pltpu.CompilerParams(
            collective_id=0, has_side_effects=True, vmem_limit_bytes=60 * 1024 * 1024
        ),
    )(hidden, down_weight, slot_gate, slot_owner, slot_row, block_count)
    return pl.pallas_call(
        functools.partial(finish, PIECE),
        out_shape=jax.ShapeDtypeStruct((TOK_DEV, width), jnp.bfloat16),
        in_specs=[vmem] * 3,
        out_specs=hbm,
        scratch_shapes=[pltpu.VMEM((TOK_DEV, width), jnp.bfloat16), dma((pieces,))],
        compiler_params=pltpu.CompilerParams(vmem_limit_bytes=8 * 1024 * 1024),
    )(*held)


def body(hidden, down_weight, *slot_data):
    groups, columns = lax.axis_size("grp"), lax.axis_size("ep")
    slots, depth = hidden.shape[2:]
    width = down_weight.shape[2]
    held = 2 * (depth * width + groups * slots * (depth + 2 * width))
    even = groups == PLANES and columns > 1 and width % (2 * PIECE) == 0
    fits = held <= VMEM_ROOM and even
    chosen = kernel_body if fits else exchange_body
    return chosen(hidden, down_weight, *slot_data)


def solution(mesh):
    in_specs = (
        P("grp", "ep", None, None),
        P("ep", None, None),
        P("grp", "ep", None),
        P("grp", "ep", None),
        P("grp", "ep", None),
        P("grp", "ep", None),
    )
    out_specs = P(("grp", "ep"), None)
    return jax.shard_map(body, mesh=mesh, in_specs=in_specs, out_specs=out_specs, check_vma=False)
```

```python
import functools

import jax
import jax.numpy as jnp
from jax import lax
from jax.experimental import pallas as pl
from jax.experimental.pallas import tpu as pltpu
from jax.sharding import PartitionSpec as P

TOK_DEV = 32
LANES = 128
PIECE = 1024
PLANES = 4
COLUMNS = 8
VMEM_ROOM = 48 * 1024 * 1024
MESH = pl.DeviceIdType.MESH


def exchange_body(hidden, down_weight, slot_gate, slot_owner, slot_row, block_count):
    columns = lax.axis_size("ep")
    slot_total = hidden.shape[2]
    send = slot_total // columns
    product = jnp.dot(hidden[0, 0], down_weight[0], preferred_element_type=jnp.float32)
    within = jnp.arange(slot_total) % send
    limits = jnp.repeat(block_count[0, 0], send)
    live = (within < limits).astype(jnp.float32)
    scaled = (product * (slot_gate[0, 0] * live)[:, None]).astype(jnp.bfloat16)
    local_index = slot_owner[0, 0] * TOK_DEV + slot_row[0, 0]
    arrived, arrived_index = (
        lax.all_to_all(scaled, "ep", split_axis=0, concat_axis=0, tiled=True),
        lax.all_to_all(local_index, "ep", split_axis=0, concat_axis=0, tiled=True),
    )
    wanted = jnp.arange(lax.axis_size("grp") * TOK_DEV)
    table = (wanted[:, None] == arrived_index[None, :]).astype(jnp.bfloat16)
    return lax.psum_scatter(
        jnp.dot(table, arrived, preferred_element_type=jnp.float32).astype(jnp.bfloat16),
        "grp",
        scatter_dimension=0,
        tiled=True,
    )


def partner(me, n, k):
    if n & (n - 1):
        return lax.rem(me + n - k, n), lax.rem(me + k, n)
    other, bit = 0, 1
    while bit < n:
        mine = lax.rem(me // bit, 2)
        other = other + bit * (1 - mine if k & bit else mine)
        bit *= 2
    return other, other


def local_cols(group, width, start, size):
    at = lax.rem(start + lax.rem(group, 2) * (width // 2), width)
    return pl.ds(pl.multiple_of(at, size), size)


def kernel(
    groups, columns, send, piece,
    hidden_ref, weight_ref, gate_ref, owner_ref, row_ref, count_ref,
    sums, last_rows, last_table,
    gate, owner, row, count, weight, rows_in, meta,
    out_early, out_late, in_early, in_late, pair_places, places, swap_out, swap_in,
    load_sem, weight_sem, corner, hid_send, hid_recv, meta_send, meta_recv,
    row_send, row_recv, place_send, place_recv, swap_send, swap_recv,
):
    group, column = lax.axis_index("grp"), lax.axis_index("ep")
    slots, width = hidden_ref.shape[2], weight_ref.shape[2]
    half = width // 2
    last = groups - 1
    total = columns * send
    pair = group + 1 - 2 * lax.rem(group, 2)
    pair_base = group - lax.rem(group, 2)
    far, far_pair = last - group, last - pair
    end = group == last
    sources = [group, pair, jnp.where(end, far_pair, far), jnp.where(end, far, far_pair)]
    column_steps = [6, 7, 4, 5, 2, 3, 1]

    def weight_copy(j):
        return pltpu.make_async_copy(
            weight_ref.at[0, :, local_cols(group, width, j * piece, piece)],
            weight.at[:, pl.ds(j * piece, piece)],
            weight_sem.at[j],
        )

    loads = [
        pltpu.make_async_copy(hidden_ref.at[0, 0], rows_in.at[group], load_sem.at[4]),
        pltpu.make_async_copy(gate_ref.at[0], gate, load_sem.at[0]),
        pltpu.make_async_copy(owner_ref.at[0], owner, load_sem.at[1]),
        pltpu.make_async_copy(row_ref.at[0], row, load_sem.at[2]),
        pltpu.make_async_copy(count_ref.at[0], count, load_sem.at[3]),
    ]
    for load in loads:
        load.start()

    barrier = pltpu.get_barrier_semaphore()
    near_steps = [k for k in column_steps if k // 2 in (0, 1, 2)]
    for k in near_steps:
        pl.semaphore_signal(
            barrier, inc=1, device_id=(group, partner(column, columns, k)[0]), device_id_type=MESH
        )
    pl.semaphore_signal(barrier, inc=1, device_id=(pair, column), device_id_type=MESH)

    @pl.when(group < last)
    def greet_far():
        pl.semaphore_signal(barrier, inc=1, device_id=(far, column), device_id_type=MESH)

    for load in loads:
        load.wait()
    for j in range(width // piece):
        weight_copy(j).start()
    lane = lax.broadcasted_iota(jnp.int32, (1, slots), 1)
    limit = jnp.zeros((1, slots), jnp.int32)
    for q in range(columns):
        limit = jnp.where(lane // send == q, count[:, q:q + 1], limit)
    scale = jnp.where(lane % send < limit, gate[...], 0.0)
    meta[group] = jnp.zeros(meta.shape[1:], jnp.float32)
    meta[group, 0, :, :slots] = scale
    meta[group, 1, :, :slots] = (owner[...] * TOK_DEV + row[...]).astype(jnp.float32)

    pl.semaphore_wait(barrier, len(near_steps) + 1 + jnp.where(group > 0, 1, 0))

    def share_copies(at, to, slot=None):
        slot = at if slot is None else slot
        return [
            pltpu.make_async_remote_copy(
                src_ref=held.at[at], dst_ref=held.at[at],
                send_sem=sent.at[slot], recv_sem=landed.at[at],
                device_id=(to, column), device_id_type=MESH,
            )
            for held, sent, landed in ((meta, meta_send, meta_recv), (rows_in, hid_send, hid_recv))
        ]

    def share(at, to, slot=None):
        for copy in share_copies(at, to, slot):
            copy.start()

    def wait_shared(at):
        for copy in share_copies(at, at):
            copy.wait_recv()

    def wait_sent(slot):
        for copy in share_copies(group, pair, slot):
            copy.wait_send()

    def rows_out(k):
        return out_early.at[k] if k < 2 else out_late.at[k - 2]

    def rows_at(k):
        return in_early.at[k] if k < 2 else last_rows if k == last else in_late.at[k - 2]

    def row_copy(k, m, j, batch):
        to = partner(column, columns, m)[0]
        cols = pl.ds(j * piece, batch * piece)
        return pltpu.make_async_remote_copy(
            src_ref=rows_out(k).at[to, :, cols], dst_ref=rows_at(k).at[column, :, cols],
            send_sem=row_send.at[k], recv_sem=row_recv.at[k],
            device_id=(group, to), device_id_type=MESH,
        )

    def all_rows(k):
        return pltpu.make_async_remote_copy(
            src_ref=rows_out(k).at[pl.ds(0, columns - 1)],
            dst_ref=rows_at(k).at[pl.ds(0, columns - 1)],
            send_sem=row_send.at[k], recv_sem=row_recv.at[k],
            device_id=(group, partner(column, columns, 1)[0]), device_id_type=MESH,
        )

    def place_copy(k, m):
        src = meta.at[sources[k], 1] if k > 1 else meta.at[pl.ds(pair_base, 2), 1]
        dst = places.at[k - 2, column] if k > 1 else pair_places.at[column]
        return pltpu.make_async_remote_copy(
            src_ref=src, dst_ref=dst,
            send_sem=place_send.at[k - 1], recv_sem=place_recv.at[k - 1],
            device_id=(group, partner(column, columns, m)[0]), device_id_type=MESH,
        )

    def all_places(k):
        some = (places.at[k - 2] if k > 1 else pair_places).at[pl.ds(0, columns - 1)]
        return pltpu.make_async_remote_copy(
            src_ref=some, dst_ref=some,
            send_sem=place_send.at[k - 1], recv_sem=place_recv.at[k - 1],
            device_id=(group, partner(column, columns, 1)[0]), device_id_type=MESH,
        )

    def swap_copy(j):
        cols = pl.ds(j * piece, piece)
        return pltpu.make_async_remote_copy(
            src_ref=swap_out.at[:, cols], dst_ref=swap_in.at[:, cols],
            send_sem=swap_send.at[j], recv_sem=swap_recv.at[j],
            device_id=(pair, column), device_id_type=MESH,
        )

    @pl.when(group > 0)
    def share_far():
        share(group, far, groups)

    share(group, pair)
    pl.semaphore_signal(
        corner, inc=1, device_id=(group, partner(column, columns, 2)[0]), device_id_type=MESH
    )
    eye = lax.broadcasted_iota(jnp.int32, (slots, slots), 0) == lax.broadcasted_iota(
        jnp.int32, (slots, slots), 1
    )
    lanes = meta.shape[3]
    picked = lax.broadcasted_iota(jnp.int32, (lanes, total), 0) == (
        column * send + lax.broadcasted_iota(jnp.int32, (lanes, total), 1) % send
    )
    picked = picked.astype(jnp.float32)
    mine = lax.broadcasted_iota(jnp.int32, (columns, total), 0) == (
        lax.broadcasted_iota(jnp.int32, (columns, total), 1) // send
    )
    token = lax.broadcasted_iota(jnp.int32, (TOK_DEV, total), 0)

    def table_of(found, owners):
        index = jnp.dot(
            found, picked, precision=lax.Precision.HIGHEST, preferred_element_type=jnp.float32
        )
        index = jnp.sum(jnp.where(mine, index, 0.0), axis=0, keepdims=True)
        return [
            ((owner_group * TOK_DEV + token).astype(jnp.float32) == index).astype(jnp.bfloat16)
            for owner_group in owners
        ]

    def block(k, cols):
        return jnp.concatenate([rows_at(k)[e, :, cols] for e in range(columns)], axis=0)

    def early_sums():
        all_places(1).wait_recv()
        both = []
        for k in range(2):
            found = pair_places[:, sources[k] - pair_base, 0]
            both.append(jnp.concatenate(table_of(found, (group, pair)), axis=0))
        table = jnp.concatenate(both, axis=1)
        for k in range(2):
            all_rows(k).wait_recv()
        for j in range(half // piece):
            cols = slice(j * piece, (j + 1) * piece)
            rows = jnp.concatenate([block(0, cols), block(1, cols)], axis=0)
            rows = jnp.dot(table, rows, preferred_element_type=jnp.float32)
            swap_out[:, cols] = rows[TOK_DEV:].astype(jnp.bfloat16)
            swap_copy(j).start()
            sums[:, cols] = rows[:TOK_DEV]

    def compute(k):
        factor = jnp.sum(jnp.where(eye, meta[sources[k], 0, :, :slots], 0.0), axis=1, keepdims=True)
        def product(j):
            if k == 0 or k == 2 and j >= half // piece:
                weight_copy(j).wait()
            cols = slice(j * piece, (j + 1) * piece)
            return jnp.dot(rows_in[sources[k]], weight[:, cols], preferred_element_type=jnp.float32)

        steps = (half if k < 2 else width) // piece
        ahead = product(0)
        for j in range(steps):
            scaled = ahead * factor
            if j + 1 < steps:
                ahead = product(j + 1)
            if k == 0 and j == 0:
                pl.semaphore_wait(corner, 1)
            cols = slice(j * piece, (j + 1) * piece)
            for q in range(columns):
                rows_out(k)[q, :, cols] = scaled[q * send:(q + 1) * send].astype(jnp.bfloat16)
            for m in column_steps:
                row_copy(k, m, j, 1).start()
        rows_at(k)[column] = rows_out(k)[column]

    def take_pair():
        wait_shared(sources[1])

        @pl.when(group == 1)
        def forward_pair():
            share(sources[1], far)

        for m in column_steps:
            place_copy(1, m).start()
        pair_places[column] = meta[pl.ds(pair_base, 2), 1]
        compute(1)

    def take_third():
        wait_shared(sources[2])

        @pl.when(group < last)
        def forward_third():
            share(sources[2], pair)

        for m in column_steps:
            place_copy(2, m).start()
        places[0, column] = meta[sources[2], 1]
        compute(2)

    compute(0)

    @pl.when(group != last - 1)
    def pair_first():
        take_pair()
        take_third()

    @pl.when(group == last - 1)
    def third_first():
        take_third()
        wait_shared(sources[last])
        share(sources[last], pair)
        take_pair()

    @pl.when(lax.rem(group, 2) == 1)
    def early_first():
        early_sums()

    @pl.when(group != last - 1)
    def wait_last():
        wait_shared(sources[last])

    for m in column_steps:
        place_copy(last, m).start()
    places[last - 2, column] = meta[sources[last], 1]
    compute(last)

    @pl.when(lax.rem(group, 2) == 0)
    def early_after():
        early_sums()

    tables = []
    for k in range(2, groups):
        all_places(k).wait_recv()
        tables.append(table_of(places[k - 2, :, 0], (group,))[0])
    last_table[...] = tables[-1]
    for k in range(2, last):
        all_rows(k).wait_recv()
        if k == 2:
            for j in range(half // piece):
                swap_copy(j).wait_recv()
        for j in range(width // piece):
            cols = slice(j * piece, (j + 1) * piece)
            rows = jnp.dot(tables[k - 2], block(k, cols), preferred_element_type=jnp.float32)
            if k > 2 or j < half // piece:
                sums[:, cols] = sums[:, cols] + rows
            else:
                swapped = swap_in[:, j * piece - half:(j + 1) * piece - half]
                sums[:, cols] = swapped.astype(jnp.float32) + rows

    wait_sent(group)

    @pl.when(group > 0)
    def sent_far():
        wait_sent(groups)

    @pl.when(group == 1)
    def sent_first():
        wait_sent(sources[1])

    @pl.when(group < last)
    def sent_second():
        wait_sent(sources[2])

    @pl.when(group == last - 1)
    def sent_last():
        wait_sent(sources[last])

    for k in range(1, groups):
        all_places(k).wait_send()
    for j in range(half // piece):
        swap_copy(j).wait_send()
    all_rows(last).wait_recv()
    for k in range(groups):
        all_rows(k).wait_send()


def finish(piece, sums, last_rows, last_table, out_ref, result, store_sem):
    group = lax.axis_index("grp")
    columns, width = last_rows.shape[0], last_rows.shape[2]
    copies = []
    for j in range(width // piece):
        cols = slice(j * piece, (j + 1) * piece)
        block = jnp.concatenate([last_rows[e, :, cols] for e in range(columns)], axis=0)
        rows = jnp.dot(last_table[...], block, preferred_element_type=jnp.float32)
        result[:, cols] = (sums[:, cols] + rows).astype(out_ref.dtype)
        copy = pltpu.make_async_copy(
            result.at[:, cols],
            out_ref.at[:, local_cols(group, width, j * piece, piece)],
            store_sem.at[j],
        )
        copy.start()
        copies.append(copy)
    for copy in copies:
        copy.wait()


def kernel_body(hidden, down_weight, slot_gate, slot_owner, slot_row, block_count):
    groups, columns = lax.axis_size("grp"), lax.axis_size("ep")
    slots, depth = hidden.shape[2:]
    width = down_weight.shape[2]
    send = slots // columns
    lanes = -(-slots // LANES) * LANES
    pieces, halves = width // PIECE, width // 2 // PIECE
    hbm = pl.BlockSpec(memory_space=pltpu.HBM)
    vmem = pl.BlockSpec(memory_space=pltpu.VMEM)
    dma = pltpu.SemaphoreType.DMA
    held = pl.pallas_call(
        functools.partial(kernel, groups, columns, send, PIECE),
        out_shape=(
            pltpu.VMEM((TOK_DEV, width), jnp.float32),
            pltpu.VMEM((columns, send, width), jnp.bfloat16),
            pltpu.VMEM((TOK_DEV, columns * send), jnp.bfloat16),
        ),
        in_specs=[hbm] * 6,
        out_specs=(vmem,) * 3,
        scratch_shapes=[
            pltpu.VMEM((1, slots), jnp.float32),
            pltpu.VMEM((1, slots), jnp.int32),
            pltpu.VMEM((1, slots), jnp.int32),
            pltpu.VMEM((1, columns), jnp.int32),
            pltpu.VMEM((depth, width), jnp.bfloat16),
            pltpu.VMEM((groups, slots, depth), jnp.bfloat16),
            pltpu.VMEM((groups, 2, 1, lanes), jnp.float32),
            pltpu.VMEM((2, columns, send, width // 2), jnp.bfloat16),
            pltpu.VMEM((groups - 2, columns, send, width), jnp.bfloat16),
            pltpu.VMEM((2, columns, send, width // 2), jnp.bfloat16),
            pltpu.VMEM((groups - 3, columns, send, width), jnp.bfloat16),
            pltpu.VMEM((columns, 2, 1, lanes), jnp.float32),
            pltpu.VMEM((groups - 2, columns, 1, lanes), jnp.float32),
            pltpu.VMEM((TOK_DEV, width // 2), jnp.bfloat16),
            pltpu.VMEM((TOK_DEV, width // 2), jnp.bfloat16),
            dma((5,)), dma((pieces,)), pltpu.SemaphoreType.REGULAR,
            dma((groups + 1,)), dma((groups,)), dma((groups + 1,)), dma((groups,)),
            dma((groups,)), dma((groups,)), dma((groups - 1,)), dma((groups - 1,)),
            dma((halves,)), dma((halves,)),
        ],
        compiler_params=pltpu.CompilerParams(
            collective_id=0, has_side_effects=True, vmem_limit_bytes=60 * 1024 * 1024
        ),
    )(hidden, down_weight, slot_gate, slot_owner, slot_row, block_count)
    return pl.pallas_call(
        functools.partial(finish, PIECE),
        out_shape=jax.ShapeDtypeStruct((TOK_DEV, width), jnp.bfloat16),
        in_specs=[vmem] * 3,
        out_specs=hbm,
        scratch_shapes=[pltpu.VMEM((TOK_DEV, width), jnp.bfloat16), dma((pieces,))],
        compiler_params=pltpu.CompilerParams(vmem_limit_bytes=8 * 1024 * 1024),
    )(*held)


def body(hidden, down_weight, *slot_data):
    groups, columns = lax.axis_size("grp"), lax.axis_size("ep")
    slots, depth = hidden.shape[2:]
    width = down_weight.shape[2]
    held = 2 * (depth * width + groups * slots * (depth + 2 * width))
    even = groups == PLANES and columns == COLUMNS and width % (2 * PIECE) == 0
    fits = held <= VMEM_ROOM and even
    chosen = kernel_body if fits else exchange_body
    return chosen(hidden, down_weight, *slot_data)


def solution(mesh):
    in_specs = (
        P("grp", "ep", None, None),
        P("ep", None, None),
        P("grp", "ep", None),
        P("grp", "ep", None),
        P("grp", "ep", None),
        P("grp", "ep", None),
    )
    out_specs = P(("grp", "ep"), None)
    return jax.shard_map(body, mesh=mesh, in_specs=in_specs, out_specs=out_specs, check_vma=False)
```
